256 devices in a mesh: blk: 64 (over x, y_lo, z), grp: 4 (over y_hi, core).
Axes of the slice: x: 4, y: 4 (y_hi: 2, y_lo: 2; y = y_hi * 2 + y_lo), z: 8, core: 2. Of those that a mesh axis runs over, the one named last changes fastest.
Arguments:
- sources: bfloat16 [65536, 256], P('blk'), may hold values from -64 to 64
- positive: int32 [65536], P('blk'), may hold values from 0 to 65535
- src_part: int32 [65536], P('blk'), may hold values from 0 to 7
- destinations: bfloat16 [65536, 256], P(('blk', 'grp')), may hold values from -8 to 8
- dst_part: int32 [65536], P(('blk', 'grp')), may hold values from 0 to 7
Outputs:
- loss: float32 [65536], P('blk')
The draws below stay inside these ranges and needn't reach their ends.
All inputs are finite; a program needn't handle non-finite values.
Results may differ from the reference program's by a relative error of at most 0.0003.
Values may be sent and summed in bfloat16 or wider, within the bound.
A program may use at most 192 MiB of HBM per device.

```python
import jax
import jax.numpy as jnp
from jax import lax

H = 256
SRC_DEV = 1024
PARTS_SIZE = 8
NSRC = 65536
NDST = 65536
N_BLK = 64


def joint_draw(key):
    keys = jax.random.split(jax.random.fold_in(key, 7), 2)
    src = jax.random.normal(keys[0], (NSRC, H), jnp.float32)
    dst = jax.random.normal(keys[1], (NDST, H), jnp.float32) * H ** (-0.5)
    return (jnp.clip(src, -64.0, 64.0), jnp.clip(dst, -8.0, 8.0))


def draw_sources(key, part):
    return joint_draw(key)[0].astype(jnp.bfloat16)


def draw_destinations(key, part):
    return joint_draw(key)[1].astype(jnp.bfloat16)


def touch_ends(result, own_key, smallest, largest):
    longest = result.shape.index(max(result.shape))
    spots = []
    for shift in (0, 1):
        where = [jax.random.randint(jax.random.fold_in(own_key, axis), (), 0, length) for axis, length in enumerate(result.shape)]
        where[longest] = (where[longest] + shift) % result.shape[longest]
        spots.append(tuple(where))
    return result.at[spots[0]].set(smallest).at[spots[1]].set(largest)


def setup_inputs(seed: int = 0) -> dict:
    key_list = jax.random.split(jax.random.key(seed), 6)
    sources = draw_sources(jax.random.fold_in(key_list[5], 71), 0)
    positive = touch_ends(jax.random.randint(key_list[1], (NSRC,), 0, NDST), jax.random.fold_in(key_list[1], 1), 0, NDST - 1).astype(jnp.int32)
    src_part = touch_ends(jax.random.randint(key_list[2], (NSRC,), 0, PARTS_SIZE), jax.random.fold_in(key_list[2], 1), 0, PARTS_SIZE - 1).astype(jnp.int32)
    destinations = draw_destinations(jax.random.fold_in(key_list[5], 71), 0)
    dst_part = touch_ends(jax.random.randint(key_list[4], (NDST,), 0, PARTS_SIZE), jax.random.fold_in(key_list[4], 1), 0, PARTS_SIZE - 1).astype(jnp.int32)
    return dict(sources=sources, positive=positive, src_part=src_part, destinations=destinations, dst_part=dst_part)


SCALE = 3.0
NEG = -1.0e30


def reference(sources, positive, src_part, destinations, dst_part):
    columns = jnp.arange(NDST, dtype=jnp.int32)
    src_blocks = sources.reshape(N_BLK, SRC_DEV, H)
    pos_blocks = positive.reshape(N_BLK, SRC_DEV)
    part_blocks = src_part.reshape(N_BLK, SRC_DEV)

    def one_block(item):
        rows, pos, part = item
        logits = SCALE * lax.dot_general(rows, destinations, (((1,), (1,)), ((), ())), preferred_element_type=jnp.float32)
        is_pos = columns[None, :] == pos[:, None]
        keep = (dst_part[None, :] != part[:, None]) | is_pos
        masked = jnp.where(keep, logits, NEG)
        top = jnp.max(masked, axis=1)
        total = jnp.sum(jnp.where(keep, jnp.exp(masked - top[:, None]), jnp.float32(0.0)), axis=1)
        pos_logit = jnp.sum(jnp.where(is_pos, logits, jnp.float32(0.0)), axis=1)
        return top + jnp.log(total) - pos_logit

    losses = lax.map(one_block, (src_blocks, pos_blocks, part_blocks))
    return losses.reshape(NSRC)
```

```python
import jax
import jax.numpy as jnp
from jax import lax
from jax.experimental import pallas as pl
from jax.experimental.pallas import tpu as pltpu
from jax.sharding import Mesh
from jax.sharding import PartitionSpec as P

F32 = jnp.float32
BF16 = jnp.bfloat16
BLK = ("x", "yl", "z")
BLK_GRP = ("x", "yl", "z", "yh", "c")
NEG = -1e30
SCALE = 3.0
SCALE2 = SCALE * 1.4426950408889634
LN2 = 0.6931471805599453

OWN, Y, XP, XM, X2, YXP, YXM, YX2 = range(8)
ROW_DX = (0, 0, 1, 3, 2, 1, 3, 2)
ROW_DY = (0, 1, 0, 0, 0, 1, 1, 1)
COL_DZ = (0, 1, 7, 2, 6, 3, 5, 4)
META = 16
ROWS = 512
COLS = 256


def score(dots, part_ref, cc, src_part, relative, r, buf, top_of, tops, hits):
    sub = lax.broadcasted_iota(jnp.int32, (8, 128), 0).astype(F32)
    for k in range(ROWS // 128):
        lanes = slice(k * 128, (k + 1) * 128)
        own_part = jnp.broadcast_to(src_part[:, lanes], (8, 128))
        at = jnp.broadcast_to(relative[:, lanes], (8, 128)) - sub
        best = jnp.full((8, 128), NEG, F32)
        hit = hits[r, :, lanes]
        for t in range(COLS // 8):
            rows = slice(8 * t, 8 * t + 8)
            value = dots[rows, lanes]
            is_pos = at == float(8 * t)
            keep = (part_ref[cc, rows, :] != own_part) | is_pos
            masked = jnp.where(keep, value, NEG)
            hit = jnp.where(is_pos, value, hit)
            best = jnp.maximum(best, masked)
            buf[rows, lanes] = masked
        best = jnp.maximum(best, tops[r, :, lanes])
        tops[r, :, lanes] = best
        top_of[:, lanes] = best
        hits[r, :, lanes] = hit


def accumulate(r, buf, top_of, sum_tops, sums):
    for k in range(ROWS // 128):
        lanes = slice(k * 128, (k + 1) * 128)
        top = top_of[:, lanes]
        parts = [jnp.zeros((8, 128), F32), jnp.zeros((8, 128), F32)]
        for t in range(COLS // 8):
            parts[t % 2] = parts[t % 2] + jnp.exp2((buf[8 * t : 8 * t + 8, lanes] - top) * SCALE2)
        before = sum_tops[r, :, lanes]
        sums[r, :, lanes] = sums[r, :, lanes] * jnp.exp2((before - top) * SCALE2) + (parts[0] + parts[1])
        sum_tops[r, :, lanes] = top


def kernel(
    src_ref, pos_ref, spart_ref, dst_ref, dpart_ref, out_ref,
    rbuf, cbuf, part, buf_a, buf_b, top_a, top_b, tops, sum_tops, sums, hits, given, got,
    local_sem, send_sem, rrecv, crecv, precv, fsend, frecv,
):
    x, yl, z = lax.axis_index("x"), lax.axis_index("yl"), lax.axis_index("z")
    yh, c = lax.axis_index("yh"), lax.axis_index("c")
    nx, nz = lax.axis_size("x"), lax.axis_size("z")
    y = yh * 2 + yl
    ny = 4

    def ring(value, step, size):
        return lax.rem(value + step + size, size)

    y_next, y_prev = ring(y, 1, ny), ring(y, -1, ny)
    xp, xm = {"x": ring(x, 1, nx)}, {"x": ring(x, -1, nx)}
    zp, zm = {"z": ring(z, 1, nz)}, {"z": ring(z, -1, nz)}
    yp = {"yh": y_next // 2, "yl": lax.rem(y_next, 2)}
    ym = {"yh": y_prev // 2, "yl": lax.rem(y_prev, 2)}
    mate = {"c": 1 - c}

    load_rows = pltpu.make_async_copy(
        src_ref.at[pl.ds(pl.multiple_of(c * ROWS, ROWS), ROWS)], rbuf.at[OWN, pl.ds(META, ROWS)], local_sem.at[0]
    )
    load_cols = pltpu.make_async_copy(dst_ref, cbuf.at[0, pl.ds(META, COLS)], local_sem.at[1])
    load_rows.start()
    load_cols.start()

    barrier = pltpu.get_barrier_semaphore()
    greeted = [zp, zm]
    for dx in range(4):
        for dy in range(4):
            for dc in range(2):
                if dx or dy or dc:
                    there = ring(y, dy, ny)
                    greeted.append(
                        {"x": ring(x, dx, nx), "yh": there // 2, "yl": lax.rem(there, 2), "c": lax.rem(c + dc, 2)}
                    )
    for peer in greeted:
        pl.semaphore_signal(barrier, inc=1, device_id=peer, device_id_type=pl.DeviceIdType.MESH)

    own_pos = jnp.where(c == 0, pos_ref[0:2, :], pos_ref[2:4, :])
    own_part = jnp.where(c == 0, spart_ref[0:2, :], spart_ref[2:4, :])
    high = own_pos // 256
    meta = jnp.concatenate(
        [high.astype(F32), (own_pos - high * 256).astype(F32), own_part.astype(F32), jnp.zeros((10, 256), F32)], axis=0
    )
    rbuf[OWN, 0:META, :] = meta.astype(BF16)
    cbuf[0, 0:META, :] = jnp.broadcast_to(dpart_ref[...].astype(F32), (META, 256)).astype(BF16)
    tops[...] = jnp.full(tops.shape, NEG, F32)
    sum_tops[...] = jnp.full(tops.shape, NEG, F32)
    sums[...] = jnp.zeros(tops.shape, F32)
    hits[...] = jnp.zeros(tops.shape, F32)

    load_rows.wait()
    load_cols.wait()
    pl.semaphore_wait(barrier, len(greeted))

    sent = []

    def send(src, dst, sem, peer):
        copy = pltpu.make_async_remote_copy(
            src_ref=src, dst_ref=dst, send_sem=send_sem.at[len(sent)], recv_sem=sem,
            device_id=peer, device_id_type=pl.DeviceIdType.MESH,
        )
        copy.start()
        sent.append(copy)

    def arrived(ref, sem):
        pltpu.make_async_remote_copy(
            src_ref=ref, dst_ref=ref, send_sem=send_sem.at[0], recv_sem=sem,
            device_id=mate, device_id_type=pl.DeviceIdType.MESH,
        ).wait_recv()

    def row_chunk(slot, chunk):
        return rbuf.at[slot, pl.ds(272 * chunk, 272 - 16 * chunk)]

    def send_rows(slot, chunk, to, peer):
        send(row_chunk(slot, chunk), row_chunk(to, chunk), rrecv.at[to, chunk], peer)

    def rows_arrived(slot, chunk):
        arrived(row_chunk(slot, chunk), rrecv.at[slot, chunk])

    def col_chunk(d, chunk):
        return cbuf.at[2 * d, pl.ds(144 * chunk, 144 - 16 * chunk)]

    def send_cols(d, chunk, to, peer):
        send(col_chunk(d, chunk), col_chunk(to, chunk), crecv.at[to, chunk], peer)

    def cols_arrived(d, chunk):
        arrived(col_chunk(d, chunk), crecv.at[d, chunk])

    def share(d):
        send(cbuf.at[2 * d], cbuf.at[2 * d + 1], precv.at[d], mate)

    def spread_part(cc):
        line = cbuf[cc, 0:META, :].astype(F32)[0:1, :]
        for k in range(2):
            part[cc, 128 * k : 128 * k + 128, :] = jnp.broadcast_to(line[:, 128 * k : 128 * k + 128], (128, 128)).T

    def shared_arrived(d):
        arrived(cbuf.at[2 * d + 1], precv.at[d])
        spread_part(2 * d + 1)

    def first(r, cc, buf, top_of):
        d = cc // 2
        step = lax.div(d + 1, 2)
        dz = jnp.where(lax.rem(d, 2) == 1, step, nz - step)
        core = jnp.where(lax.rem(cc, 2) == 0, c, 1 - c)
        blk = (x * 2 + yl) * nz + lax.rem(z + dz, nz)
        base = ((blk * 2 + yh) * 2 + core) * COLS
        line = rbuf[r, 0:META, :].astype(F32)
        src_part = jnp.concatenate([line[4:5], line[5:6]], axis=1)
        positive = jnp.concatenate([line[0:1], line[1:2]], axis=1) * 256.0
        positive = positive + jnp.concatenate([line[2:3], line[3:4]], axis=1)
        dots = lax.dot_general(
            cbuf[cc, META : META + COLS, :], rbuf[r, META : META + ROWS, :],
            (((1,), (1,)), ((), ())), preferred_element_type=F32,
        )
        score(dots, part, cc, src_part, positive - base.astype(F32), r, buf, top_of, tops, hits)

    def tiles(r0, r1, c0, c1, stride=1):
        width = -(-(c1 - c0) // stride)
        count = (r1 - r0) * width

        def where(i):
            return r0 + lax.div(i, width), c0 + stride * lax.rem(i, width)

        def one(i, buf, top_of):
            first(*where(i), buf, top_of)

        def two(i, buf, top_of):
            accumulate(where(i)[0], buf, top_of, sum_tops, sums)

        assert count % 2 == 0 or count == 1
        if count == 1:
            one(jnp.int32(0), buf_a, top_a)
            two(jnp.int32(0), buf_a, top_a)
            return
        one(jnp.int32(0), buf_a, top_a)

        def pair(j, carry):
            i = 2 * j
            one(i + 1, buf_b, top_b)
            two(i, buf_a, top_a)
            one(i + 2, buf_a, top_a)
            two(i + 1, buf_b, top_b)
            return carry

        lax.fori_loop(0, count // 2 - 1, pair, 0)
        one(jnp.int32(count - 1), buf_b, top_b)
        two(jnp.int32(count - 2), buf_a, top_a)
        two(jnp.int32(count - 1), buf_b, top_b)

    finals = []

    def finish(r):
        sub = lax.broadcasted_iota(jnp.int32, (8, ROWS), 0)
        top = jnp.max(tops[r], axis=0, keepdims=True)
        total = jnp.sum(sums[r] * jnp.exp2((sum_tops[r] - top) * SCALE2), axis=0, keepdims=True)
        hit = jnp.sum(hits[r], axis=0, keepdims=True)
        line = jnp.where(sub == 0, top, jnp.where(sub == 1, total, hit))
        here = x * ny + y
        if r == OWN:
            got[c, here] = line
        given[r] = line
        bx, by = ring(x, ROW_DX[r], nx), lax.rem(yl + ROW_DY[r], 2)
        for other_yh in (0, 1):
            for other_c in (0, 1):
                if r == OWN and other_yh == 0 and other_c == 0:
                    continue
                if r == OWN:
                    peer = {"yh": lax.rem(yh + other_yh, 2), "c": lax.rem(c + other_c, 2)}
                else:
                    peer = {"x": bx, "yl": by, "yh": other_yh, "c": other_c}
                copy = pltpu.make_async_remote_copy(
                    src_ref=given.at[r], dst_ref=got.at[c, here], send_sem=fsend.at[len(finals)],
                    recv_sem=frecv.at[c, here], device_id=peer, device_id_type=pl.DeviceIdType.MESH,
                )
                copy.start()
                finals.append(copy)

    for chunk in (0, 1):
        send_cols(0, chunk, 1, zm)
        send_cols(0, 1 - chunk, 2, zp)
        send_rows(OWN, chunk, XP, xm)
        send_rows(OWN, 1 - chunk, XM, xp)
        send_rows(OWN, chunk, Y, (yp, ym)[chunk])
    share(0)
    spread_part(0)
    tiles(0, 1, 0, 1)
    shared_arrived(0)
    tiles(0, 1, 1, 2)

    cols_arrived(1, 0)
    send_cols(1, 0, 3, zm)
    cols_arrived(2, 1)
    send_cols(2, 1, 4, zp)
    rows_arrived(XP, 0)
    send_rows(XP, 0, X2, xm)
    send_rows(XP, 0, YXP, yp)
    rows_arrived(XM, 1)
    send_rows(XM, 1, X2, xp)
    send_rows(XM, 1, YXM, ym)
    cols_arrived(1, 1)
    send_cols(1, 1, 3, zm)
    share(1)
    cols_arrived(2, 0)
    send_cols(2, 0, 4, zp)
    share(2)
    spread_part(2)
    spread_part(4)
    rows_arrived(Y, 0)
    rows_arrived(Y, 1)
    tiles(1, 2, 0, 2)
    tiles(0, 2, 2, 6, 2)
    shared_arrived(1)
    shared_arrived(2)
    tiles(0, 2, 3, 6, 2)

    cols_arrived(3, 0)
    send_cols(3, 0, 5, zm)
    cols_arrived(4, 1)
    send_cols(4, 1, 6, zp)
    rows_arrived(XP, 1)
    send_rows(XP, 1, YXP, ym)
    rows_arrived(XM, 0)
    send_rows(XM, 0, YXM, yp)
    cols_arrived(3, 1)
    send_cols(3, 1, 5, zm)
    share(3)
    cols_arrived(4, 0)
    send_cols(4, 0, 6, zp)
    share(4)
    tiles(2, 4, 0, 6)

    cols_arrived(5, 0)
    send_cols(5, 0, 7, zm)
    cols_arrived(6, 1)
    send_cols(6, 1, 7, zp)
    rows_arrived(X2, 0)
    send_rows(X2, 0, YX2, yp)
    rows_arrived(X2, 1)
    send_rows(X2, 1, YX2, ym)
    spread_part(6)
    spread_part(8)
    shared_arrived(3)
    shared_arrived(4)
    tiles(0, 4, 6, 10)

    cols_arrived(5, 1)
    share(5)
    cols_arrived(6, 0)
    share(6)
    tiles(4, 5, 0, 10)
    spread_part(10)
    spread_part(12)
    shared_arrived(5)
    shared_arrived(6)
    cols_arrived(7, 0)
    cols_arrived(7, 1)
    share(7)
    tiles(0, 5, 10, 14)
    spread_part(14)
    shared_arrived(7)
    tiles(0, 5, 14, 16)
    for r in range(5):
        finish(r)
    rows_arrived(YXP, 0)
    rows_arrived(YXP, 1)
    tiles(5, 6, 0, 16)
    finish(5)
    rows_arrived(YXM, 0)
    rows_arrived(YXM, 1)
    tiles(6, 7, 0, 16)
    finish(6)
    rows_arrived(YX2, 0)
    rows_arrived(YX2, 1)
    tiles(7, 8, 0, 16)
    finish(7)

    for copy in sent:
        copy.wait_send()
    for r, copy in enumerate(finals):
        copy.wait_send()
    for half in (0, 1):
        for dx in range(4):
            for dy in range(4):
                for_own = dx == 0 and dy == 0
                whose = ring(x, dx, nx) * ny + ring(y, dy, ny)
                core = lax.rem(c + half, 2)
                if not (for_own and half == 0):
                    arrived(got.at[core, whose], frecv.at[core, whose])
    for half in (0, 1):
        every = got[half]
        tops_of = every[:, 0, :]
        top = jnp.max(tops_of, axis=0, keepdims=True)
        total = jnp.sum(every[:, 1, :] * jnp.exp2((tops_of - top) * SCALE2), axis=0, keepdims=True)
        hit = jnp.sum(every[:, 2, :], axis=0, keepdims=True)
        out_ref[half : half + 1, :] = SCALE * (top - hit) + jnp.log(total)


def on_device(sources, positive, src_part, destinations, dst_part):
    vmem, anywhere = pl.BlockSpec(memory_space=pltpu.VMEM), pl.BlockSpec(memory_space=pl.ANY)
    out = pl.pallas_call(
        kernel,
        out_shape=jax.ShapeDtypeStruct((2, ROWS), F32),
        in_specs=[anywhere, vmem, vmem, anywhere, vmem],
        out_specs=vmem,
        scratch_shapes=[
            pltpu.VMEM((8, META + ROWS, 256), BF16),
            pltpu.VMEM((16, META + COLS, 256), BF16),
            pltpu.VMEM((16, COLS, 128), F32),
            pltpu.VMEM((COLS, ROWS), F32),
            pltpu.VMEM((COLS, ROWS), F32),
            pltpu.VMEM((8, ROWS), F32),
            pltpu.VMEM((8, ROWS), F32),
            pltpu.VMEM((8, 8, ROWS), F32),
            pltpu.VMEM((8, 8, ROWS), F32),
            pltpu.VMEM((8, 8, ROWS), F32),
            pltpu.VMEM((8, 8, ROWS), F32),
            pltpu.VMEM((8, 8, ROWS), F32),
            pltpu.VMEM((2, 16, 8, ROWS), F32),
            pltpu.SemaphoreType.DMA((2,)),
            pltpu.SemaphoreType.DMA((40,)),
            pltpu.SemaphoreType.DMA((8, 2)),
            pltpu.SemaphoreType.DMA((8, 2)),
            pltpu.SemaphoreType.DMA((8,)),
            pltpu.SemaphoreType.DMA((31,)),
            pltpu.SemaphoreType.DMA((2, 16)),
        ],
        compiler_params=pltpu.CompilerParams(
            collective_id=0, has_side_effects=True, vmem_limit_bytes=48 * 1024 * 1024
        ),
        name="loss",
    )(
        sources,
        positive.reshape(4, 256),
        src_part.reshape(4, 256),
        destinations,
        dst_part.reshape(1, 256),
    )
    return out.reshape(-1)


def solution(mesh):
    finer = Mesh(mesh.devices.reshape(4, 2, 8, 2, 2), ("x", "yl", "z", "yh", "c"))
    placed = (P(BLK, None), P(BLK), P(BLK), P(BLK_GRP, None), P(BLK_GRP))
    return jax.shard_map(on_device, mesh=finer, in_specs=placed, out_specs=P(BLK), check_vma=False)
```

```python
import jax
import jax.numpy as jnp
from jax import lax
from jax.experimental import pallas as pl
from jax.experimental.pallas import tpu as pltpu
from jax.sharding import Mesh
from jax.sharding import PartitionSpec as P

F32 = jnp.float32
BF16 = jnp.bfloat16
BLK = ("x", "yl", "z")
BLK_GRP = ("x", "yl", "z", "yh", "c")
NEG = -1e30
SCALE = 3.0
SCALE2 = SCALE * 1.4426950408889634
LN2 = 0.6931471805599453

OWN, Y, XP, XM, X2, YXP, YXM, YX2 = range(8)
ROW_DX = (0, 0, 1, 3, 2, 1, 3, 2)
ROW_DY = (0, 1, 0, 0, 0, 1, 1, 1)
COL_DZ = (0, 1, 7, 2, 6, 3, 5, 4)
META = 16
ROWS = 512
COLS = 256
LANES = [slice(k, k + 128) for k in range(0, ROWS, 128)]


def score(dots, part_ref, d, src_part, relative, r, buf, top_of, tops, hits):
    sub = lax.broadcasted_iota(jnp.int32, (8, 128), 0).astype(F32)
    own_part = [jnp.broadcast_to(src_part[:, lanes], (8, 128)) for lanes in LANES]
    at = [[jnp.broadcast_to(side[:, lanes], (8, 128)) - sub for lanes in LANES] for side in relative]
    best = [jnp.full((8, 128), NEG, F32) for _ in LANES]
    hit = [hits[r, :, lanes] for lanes in LANES]
    for t in range(2 * COLS // 8):
        rows = slice(8 * t, 8 * t + 8)
        side, first = divmod(8 * t, COLS)
        for k, lanes in enumerate(LANES):
            value = dots[rows, lanes]
            is_pos = at[side][k] == float(first)
            keep = (part_ref[d, rows, :] != own_part[k]) | is_pos
            masked = jnp.where(keep, value, NEG)
            hit[k] = jnp.where(is_pos, value, hit[k])
            best[k] = jnp.maximum(best[k], masked)
            buf[rows, lanes] = masked
    for k, lanes in enumerate(LANES):
        top = jnp.maximum(best[k], tops[r, :, lanes])
        tops[r, :, lanes] = top
        top_of[:, lanes] = top
        hits[r, :, lanes] = hit[k]


def accumulate(r, buf, top_of, sum_tops, sums):
    top = [top_of[:, lanes] for lanes in LANES]
    total = [jnp.zeros((8, 128), F32) for _ in LANES]
    for t in range(2 * COLS // 8):
        for k, lanes in enumerate(LANES):
            total[k] = total[k] + jnp.exp2((buf[8 * t : 8 * t + 8, lanes] - top[k]) * SCALE2)
    for k, lanes in enumerate(LANES):
        before = sum_tops[r, :, lanes]
        sums[r, :, lanes] = sums[r, :, lanes] * jnp.exp2((before - top[k]) * SCALE2) + total[k]
        sum_tops[r, :, lanes] = top[k]


def kernel(
    src_ref, pos_ref, spart_ref, dst_ref, dpart_ref, out_ref,
    pos_in, spart_in, dpart_in, rbuf, cbuf, part, buf_a, buf_b, top_a, top_b, tops, sum_tops, sums, hits, given, got,
    local_sem, send_sem, rrecv, crecv, precv, fsend, frecv,
):
    x, yl, z = lax.axis_index("x"), lax.axis_index("yl"), lax.axis_index("z")
    yh, c = lax.axis_index("yh"), lax.axis_index("c")
    nx, nz = lax.axis_size("x"), lax.axis_size("z")
    y = yh * 2 + yl
    ny = 4

    def ring(value, step, size):
        return lax.rem(value + step + size, size)

    y_next, y_prev = ring(y, 1, ny), ring(y, -1, ny)
    xp, xm = {"x": ring(x, 1, nx)}, {"x": ring(x, -1, nx)}
    zp, zm = {"z": ring(z, 1, nz)}, {"z": ring(z, -1, nz)}
    yp = {"yh": y_next // 2, "yl": lax.rem(y_next, 2)}
    ym = {"yh": y_prev // 2, "yl": lax.rem(y_prev, 2)}
    mate = {"c": 1 - c}

    load_rows = pltpu.make_async_copy(
        src_ref.at[pl.ds(pl.multiple_of(c * ROWS, ROWS), ROWS)], rbuf.at[OWN, pl.ds(META, ROWS)], local_sem.at[0]
    )
    load_cols = pltpu.make_async_copy(dst_ref, cbuf.at[0, pl.ds(META, COLS)], local_sem.at[1])
    load_rows.start()
    load_cols.start()
    load_pos = pltpu.make_async_copy(pos_ref, pos_in, local_sem.at[2])
    load_spart = pltpu.make_async_copy(spart_ref, spart_in, local_sem.at[3])
    load_dpart = pltpu.make_async_copy(dpart_ref, dpart_in, local_sem.at[4])
    load_pos.start()
    load_spart.start()
    load_dpart.start()

    barrier = pltpu.get_barrier_semaphore()
    greeted = [zp, zm]
    for dx in range(4):
        for dy in range(4):
            for dc in range(2):
                if dx or dy or dc:
                    there = ring(y, dy, ny)
                    greeted.append(
                        {"x": ring(x, dx, nx), "yh": there // 2, "yl": lax.rem(there, 2), "c": lax.rem(c + dc, 2)}
                    )
    for peer in greeted:
        pl.semaphore_signal(barrier, inc=1, device_id=peer, device_id_type=pl.DeviceIdType.MESH)

    tops[...] = jnp.full(tops.shape, NEG, F32)
    sum_tops[...] = jnp.full(tops.shape, NEG, F32)
    sums[...] = jnp.zeros(tops.shape, F32)
    hits[...] = jnp.zeros(tops.shape, F32)

    def halves(ref):
        mine = jnp.where(c == 0, ref[0:4, :], ref[4:8, :])
        return jnp.concatenate(
            [jnp.concatenate([mine[k : k + 1], mine[k + 1 : k + 2]], axis=1) for k in (0, 2)], axis=0
        )

    load_pos.wait()
    load_spart.wait()
    load_dpart.wait()
    own_pos = halves(pos_in)
    high = own_pos // 256
    meta = jnp.concatenate(
        [
            high.astype(F32),
            (own_pos - high * 256).astype(F32),
            halves(spart_in).astype(F32),
            jnp.zeros((META - 6, 256), F32),
        ],
        axis=0,
    )
    rbuf[OWN, 0:META, :] = meta.astype(BF16)
    line = jnp.concatenate([dpart_in[0:1, :], dpart_in[1:2, :]], axis=1).astype(F32)
    cbuf[0, 0:META, :] = jnp.broadcast_to(line, (META, 256)).astype(BF16)

    load_rows.wait()
    load_cols.wait()
    pl.semaphore_wait(barrier, len(greeted))

    sent = []

    def send(src, dst, sem, peer):
        copy = pltpu.make_async_remote_copy(
            src_ref=src, dst_ref=dst, send_sem=send_sem.at[len(sent)], recv_sem=sem,
            device_id=peer, device_id_type=pl.DeviceIdType.MESH,
        )
        copy.start()
        sent.append(copy)

    def arrived(ref, sem):
        pltpu.make_async_remote_copy(
            src_ref=ref, dst_ref=ref, send_sem=send_sem.at[0], recv_sem=sem,
            device_id=mate, device_id_type=pl.DeviceIdType.MESH,
        ).wait_recv()

    def row_chunk(slot, chunk):
        return rbuf.at[slot, pl.ds(272 * chunk, 272 - 16 * chunk)]

    def send_rows(slot, chunk, to, peer):
        send(row_chunk(slot, chunk), row_chunk(to, chunk), rrecv.at[to, chunk], peer)

    def rows_arrived(slot, chunk):
        arrived(row_chunk(slot, chunk), rrecv.at[slot, chunk])

    def col_chunk(d, chunk):
        return cbuf.at[d, pl.ds(144 * chunk, 144 - 16 * chunk)]

    def send_cols(d, chunk, to, peer):
        send(col_chunk(d, chunk), col_chunk(to, chunk), crecv.at[to, chunk], peer)

    def cols_arrived(d, chunk):
        arrived(col_chunk(d, chunk), crecv.at[d, chunk])

    def mates_rows(d):
        return cbuf.at[d, pl.ds(META + COLS, COLS)]

    def mates_meta(d):
        return cbuf.at[d, pl.ds(META + 2 * COLS, META)]

    def share(d):
        send(cbuf.at[d, pl.ds(META, COLS)], mates_rows(d), precv.at[d, 0], mate)
        send(cbuf.at[d, pl.ds(0, META)], mates_meta(d), precv.at[d, 1], mate)

    def shared_arrived(*slots):
        for d in slots:
            arrived(mates_rows(d), precv.at[d, 0])
            arrived(mates_meta(d), precv.at[d, 1])
        for d in slots:
            for side, at in enumerate((0, META + 2 * COLS)):
                line = cbuf[d, at : at + META, :].astype(F32)[0:1, :]
                for k in range(2):
                    first = COLS * side + 128 * k
                    part[d, first : first + 128, :] = jnp.broadcast_to(line[:, 128 * k : 128 * k + 128], (128, 128)).T

    def one(r, d, buf, top_of):
        step = lax.div(d + 1, 2)
        dz = jnp.where(lax.rem(d, 2) == 1, step, nz - step)
        blk = (x * 2 + yl) * nz + lax.rem(z + dz, nz)
        line = rbuf[r, 0:META, :].astype(F32)
        src_part = jnp.concatenate([line[4:5], line[5:6]], axis=1)
        positive = jnp.concatenate([line[0:1], line[1:2]], axis=1) * 256.0
        positive = positive + jnp.concatenate([line[2:3], line[3:4]], axis=1)
        relative = [
            positive - (((blk * 2 + yh) * 2 + core) * COLS).astype(F32) for core in (c, 1 - c)
        ]
        dots = lax.dot_general(
            cbuf[d, META : META + 2 * COLS, :], rbuf[r, META : META + ROWS, :],
            (((1,), (1,)), ((), ())), preferred_element_type=F32,
        )
        score(dots, part, d, src_part, relative, r, buf, top_of, tops, hits)

    buffers = [(buf_a, top_a), (buf_b, top_b)]
    pending = []

    def tiles(r0, r1, d0, d1):
        width = d1 - d0
        count = (r1 - r0) * width

        def row(i):
            return r0 + lax.div(i, width)

        def score_of(i, side):
            one(row(i), d0 + lax.rem(i, width), *buffers[side])

        def sum_of(r, side):
            accumulate(r, *buffers[side], sum_tops, sums)

        def single(i):
            score_of(jnp.int32(i), 1)
            sum_of(pending[0], 0)
            buffers.reverse()
            pending[:] = [r0 + i // width]

        if not pending:
            assert count == 1
            score_of(jnp.int32(0), 0)
            pending[:] = [r0]
            return
        if count == 1:
            single(0)
            return
        assert count % 2 == 0
        pairs = count // 2
        last = pending[0]

        def pair(j, carry):
            i = 2 * j
            new = lax.div(pairs - j, pairs)
            score_of(i, 1)
            sum_of(new * last + (1 - new) * row(i - 1 + new), 0)
            score_of(i + 1, 0)
            sum_of(row(i), 1)
            return carry

        lax.fori_loop(0, pairs, pair, 0)
        pending[:] = [r0 + (count - 1) // width]

    finals = []

    def finish(r):
        sub = lax.broadcasted_iota(jnp.int32, (8, ROWS), 0)
        top = jnp.max(tops[r], axis=0, keepdims=True)
        total = jnp.sum(sums[r] * jnp.exp2((sum_tops[r] - top) * SCALE2), axis=0, keepdims=True)
        hit = jnp.sum(hits[r], axis=0, keepdims=True)
        line = jnp.where(sub == 0, top, jnp.where(sub == 1, total, hit))
        here = x * ny + y
        if r == OWN:
            got[c, here] = line
        given[r] = line
        bx, by = ring(x, ROW_DX[r], nx), lax.rem(yl + ROW_DY[r], 2)
        for other_yh in (0, 1):
            for other_c in (0, 1):
                if r == OWN and other_yh == 0 and other_c == 0:
                    continue
                if r == OWN:
                    peer = {"yh": lax.rem(yh + other_yh, 2), "c": lax.rem(c + other_c, 2)}
                else:
                    peer = {"x": bx, "yl": by, "yh": other_yh, "c": other_c}
                copy = pltpu.make_async_remote_copy(
                    src_ref=given.at[r], dst_ref=got.at[c, here], send_sem=fsend.at[len(finals)],
                    recv_sem=frecv.at[c, here], device_id=peer, device_id_type=pl.DeviceIdType.MESH,
                )
                copy.start()
                finals.append(copy)

    for chunk in (0, 1):
        send_cols(0, chunk, 1, zm)
        send_cols(0, 1 - chunk, 2, zp)
        send_rows(OWN, chunk, XP, xm)
        send_rows(OWN, 1 - chunk, XM, xp)
        send_rows(OWN, chunk, Y, (yp, ym)[chunk])
    share(0)
    shared_arrived(0)
    tiles(0, 1, 0, 1)

    cols_arrived(1, 0)
    send_cols(1, 0, 3, zm)
    cols_arrived(2, 1)
    send_cols(2, 1, 4, zp)
    rows_arrived(XP, 0)
    send_rows(XP, 0, X2, xm)
    send_rows(XP, 0, YXP, yp)
    rows_arrived(XM, 1)
    send_rows(XM, 1, X2, xp)
    send_rows(XM, 1, YXM, ym)
    cols_arrived(1, 1)
    send_cols(1, 1, 3, zm)
    share(1)
    cols_arrived(2, 0)
    send_cols(2, 0, 4, zp)
    share(2)
    rows_arrived(Y, 0)
    rows_arrived(Y, 1)
    tiles(1, 2, 0, 1)
    shared_arrived(1, 2)
    tiles(0, 2, 1, 3)

    cols_arrived(3, 0)
    send_cols(3, 0, 5, zm)
    cols_arrived(4, 1)
    send_cols(4, 1, 6, zp)
    rows_arrived(XP, 1)
    send_rows(XP, 1, YXP, ym)
    rows_arrived(XM, 0)
    send_rows(XM, 0, YXM, yp)
    tiles(2, 4, 0, 3)
    cols_arrived(3, 1)
    send_cols(3, 1, 5, zm)
    share(3)
    cols_arrived(4, 0)
    send_cols(4, 0, 6, zp)
    share(4)
    rows_arrived(X2, 0)
    send_rows(X2, 0, YX2, yp)
    rows_arrived(X2, 1)
    send_rows(X2, 1, YX2, ym)
    shared_arrived(3, 4)
    tiles(0, 4, 3, 5)
    cols_arrived(5, 0)
    send_cols(5, 0, 7, zm)
    cols_arrived(6, 1)
    send_cols(6, 1, 7, zp)
    cols_arrived(5, 1)
    share(5)
    cols_arrived(6, 0)
    share(6)
    rows_arrived(YXP, 0)
    rows_arrived(YXP, 1)
    tiles(4, 6, 0, 5)
    shared_arrived(5, 6)
    tiles(2, 6, 5, 7)
    cols_arrived(7, 0)
    cols_arrived(7, 1)
    share(7)
    rows_arrived(YXM, 0)
    rows_arrived(YXM, 1)
    rows_arrived(YX2, 0)
    rows_arrived(YX2, 1)
    tiles(6, 8, 0, 7)
    shared_arrived(7)
    tiles(2, 8, 7, 8)
    tiles(0, 2, 5, 6)
    for r in range(2, 8):
        finish(r)
    tiles(0, 2, 6, 8)
    accumulate(pending[0], *buffers[0], sum_tops, sums)
    finish(OWN)
    finish(Y)

    for copy in sent:
        copy.wait_send()
    for r, copy in enumerate(finals):
        copy.wait_send()
    for half in (0, 1):
        for dx in range(4):
            for dy in range(4):
                for_own = dx == 0 and dy == 0
                whose = ring(x, dx, nx) * ny + ring(y, dy, ny)
                core = lax.rem(c + half, 2)
                if not (for_own and half == 0):
                    arrived(got.at[core, whose], frecv.at[core, whose])
    for half in (0, 1):
        every = got[half]
        tops_of = every[:, 0, :]
        top = jnp.max(tops_of, axis=0, keepdims=True)
        total = jnp.sum(every[:, 1, :] * jnp.exp2((tops_of - top) * SCALE2), axis=0, keepdims=True)
        hit = jnp.sum(every[:, 2, :], axis=0, keepdims=True)
        loss = SCALE * (top - hit) + jnp.log(total)
        for k, lanes in enumerate(LANES):
            out_ref[4 * half + k : 4 * half + k + 1, :] = loss[:, lanes]


def on_device(sources, positive, src_part, destinations, dst_part):
    vmem, anywhere = pl.BlockSpec(memory_space=pltpu.VMEM), pl.BlockSpec(memory_space=pl.ANY)
    out = pl.pallas_call(
        kernel,
        out_shape=jax.ShapeDtypeStruct((8, 128), F32),
        in_specs=[anywhere] * 5,
        out_specs=vmem,
        scratch_shapes=[
            pltpu.VMEM((8, 128), jnp.int32),
            pltpu.VMEM((8, 128), jnp.int32),
            pltpu.VMEM((2, 128), jnp.int32),
            pltpu.VMEM((8, META + ROWS, 256), BF16),
            pltpu.VMEM((8, 2 * META + 2 * COLS, 256), BF16),
            pltpu.VMEM((8, 2 * COLS, 128), F32),
            pltpu.VMEM((2 * COLS, ROWS), F32),
            pltpu.VMEM((2 * COLS, ROWS), F32),
            pltpu.VMEM((8, ROWS), F32),
            pltpu.VMEM((8, ROWS), F32),
            pltpu.VMEM((8, 8, ROWS), F32),
            pltpu.VMEM((8, 8, ROWS), F32),
            pltpu.VMEM((8, 8, ROWS), F32),
            pltpu.VMEM((8, 8, ROWS), F32),
            pltpu.VMEM((8, 8, ROWS), F32),
            pltpu.VMEM((2, 16, 8, ROWS), F32),
            pltpu.SemaphoreType.DMA((5,)),
            pltpu.SemaphoreType.DMA((48,)),
            pltpu.SemaphoreType.DMA((8, 2)),
            pltpu.SemaphoreType.DMA((8, 2)),
            pltpu.SemaphoreType.DMA((8, 2)),
            pltpu.SemaphoreType.DMA((31,)),
            pltpu.SemaphoreType.DMA((2, 16)),
        ],
        compiler_params=pltpu.CompilerParams(
            collective_id=0,
            has_side_effects=True,
            vmem_limit_bytes=63 * 1024 * 1024,
        ),
        name="loss",
    )(
        sources,
        positive.reshape(8, 128),
        src_part.reshape(8, 128),
        destinations,
        dst_part.reshape(2, 128),
    )
    return out.reshape(-1)


def solution(mesh):
    finer = Mesh(mesh.devices.reshape(4, 2, 8, 2, 2), ("x", "yl", "z", "yh", "c"))
    placed = (P(BLK, None), P(BLK), P(BLK), P(BLK_GRP, None), P(BLK_GRP))
    return jax.shard_map(on_device, mesh=finer, in_specs=placed, out_specs=P(BLK), check_vma=False)
```
